128 devices in a mesh: expert: 8 (over y, x_lo), ffn: 16 (over z, x_hi, core).
Axes of the slice: x: 4 (x_hi: 2, x_lo: 2; x = x_hi * 2 + x_lo), y: 4, z: 4, core: 2. Of those that a mesh axis runs over, the one named last changes fastest.
Arguments:
- tokens: bfloat16 [2048, 4096], P('expert'), may hold values from -6 to 6
- router_gates: float32 [2048, 2], P('expert'), may hold values from 0.1 to 1
- routes: int32 [2048, 2], P('expert'), may hold values from 0 to 7, all different within a row; in each aligned block of 256 rows (0 to 255, 256 to 511, ...) at most 128 rows name the same one
- gate_proj: bfloat16 [8, 4096, 14336], P('expert', None, 'ffn'), may hold values from -0.09375 to 0.09375
- up_proj: bfloat16 [8, 4096, 14336], P('expert', None, 'ffn'), may hold values from -0.09375 to 0.09375
- down_proj: bfloat16 [8, 14336, 4096], P('expert', 'ffn'), may hold values from -0.0625 to 0.0625
Outputs:
- mixed: bfloat16 [2048, 4096], P('expert', 'ffn')
The draws below stay inside these ranges and needn't reach their ends.
Inputs may be any that keep to these rules, and one draw needn't show every extreme that they name: `routes`: the 2 experts of a token differ. Among the tokens of one index of the expert axis (aligned blocks of 256 tokens) no expert is chosen by more than 128 tokens, and in some blocks one expert is chosen by exactly 128.
All inputs are finite; a program needn't handle non-finite values.
Results may differ from the reference program's by a relative error of at most 0.017.
Values may be sent and summed in bfloat16 or wider, within the bound.
No kernel may reach another device: no remote copies, remote signals or barrier semaphores. Data moves between devices by JAX's collectives and lax.ppermute only.
A program may use at most 128 MiB of HBM per device.

```python
import math
import jax
import jax.numpy as jnp
import numpy as np
from jax import lax

D = 4096
FF = 14336
TOP = 2
TOK_DEV = 256
EXPERTS = 8
CAP = 128
TOKENS = 2048
N_FFN = 16


def strengthened(values, rng, source, target, parts, factor):
    def block_of(dim):
        return (jnp.arange(values.shape[dim]) // (values.shape[dim] // parts)).reshape((-1,) + (1,) * (values.ndim - 1 - dim))

    one_side = jax.random.permutation(rng, parts)[block_of(target)]
    other_side = (block_of(target) + parts // 2) % parts
    return jnp.where((block_of(source) == one_side) | (block_of(source) == other_side), factor * values, values)


def steps_of(key, dims, pieces, low, high):
    loudness = 1.0
    for axis_at, shards_of in pieces:
        steps = jax.random.uniform(jax.random.fold_in(jax.random.fold_in(key, 6), axis_at), (shards_of,), jnp.float32, low / len(pieces), high / len(pieces))
        loudness = loudness * jnp.repeat(jnp.exp(steps), dims[axis_at] // shards_of).reshape((-1,) + (1,) * (len(dims) - 1 - axis_at))
    return loudness


def shared_out(key, own, number, rows, count, top, limit, lean):
    sequence = jax.random.permutation(key, count)
    crowded, ordinary = load_shares(count, rows * top, limit, lean, True), load_shares(count, rows * top, limit, lean, False)
    places = jnp.arange(count)

    def named(lengths, offset_by):
        used = int((lengths > 0).sum())
        fixed = max(1, used // 4)
        passed = fixed + (places - fixed + offset_by * (used - fixed)) % max(1, count - fixed)
        return jnp.zeros((count,), jnp.int32).at[sequence[jnp.where(places < fixed, places, passed)]].set(jnp.asarray(lengths, jnp.int32))

    lengths = jnp.where(number % 4 == 0, named(crowded, number // 4), named(ordinary, number - number // 4 - 1))
    mixed = jax.random.permutation(jax.random.fold_in(own, 3), count)
    source_of, taker = mixed[0:count // 2 * 2:2], mixed[1:count // 2 * 2:2]
    slack = jnp.minimum(lengths[source_of] - 1, limit - lengths[taker]) // 2
    slack = jnp.where((source_of == sequence[0]) | (taker == sequence[0]) | (lengths[taker] == 0), 0, jnp.maximum(slack, 0))
    passed = jax.random.randint(jax.random.fold_in(own, 4), (count // 2,), 0, 1 << 20) % (slack + 1)
    lengths = lengths.at[source_of].add(-passed).at[taker].add(passed)
    labels = jnp.searchsorted(jnp.cumsum(lengths), jnp.arange(rows * top), side="right").astype(jnp.int32)
    grid = labels.reshape(top, rows).T
    grid = grid[jax.random.permutation(jax.random.fold_in(own, 1), rows)]
    offset_by = jax.random.randint(jax.random.fold_in(own, 2), (rows, 1), 0, top)
    return jnp.take_along_axis(grid, (jnp.arange(top)[None, :] + offset_by) % top, axis=1)


def load_shares(number_of, total, reach, lean, full):
    weights = [(1 << 20) // math.isqrt(standing ** lean) + 1 for standing in range(1, number_of + 1)]
    largest = reach if full else min(reach, max(-(-total // number_of), total * weights[0] // sum(weights)))
    least = 1 if total - largest >= number_of - 1 else 0
    holding, surplus = [largest] + [least] * (number_of - 1), total - largest - least * (number_of - 1)
    while surplus > 0:
        free = [i for i in range(1, number_of) if holding[i] < largest] or [i for i in range(1, number_of) if holding[i] < reach]
        pool, budget = sum([weights[i] for i in free]), surplus
        for i in free:
            extra = min(reach - holding[i], max(1, budget * weights[i] // pool), surplus)
            holding[i] = holding[i] + extra
            surplus = surplus - extra
    return np.array(holding)


def centred(own_key, shape, deviation, most, shards=(), kind=jnp.bfloat16):
    entries = deviation * jax.random.normal(own_key, shape, jnp.float32)
    if shards:
        entries = entries * steps_of(own_key, shape, shards, -0.22, 0.18)
    return jnp.clip(entries, -most, most).astype(kind)


def gaussian_with(own_key, extent, spread, bound, cuts, heavy, kind=jnp.bfloat16):
    drawn = spread * jax.random.normal(own_key, extent, jnp.float32)
    if cuts:
        drawn = drawn * steps_of(own_key, extent, cuts, -0.22, 0.18)
    return jnp.clip(strengthened(drawn, jax.random.fold_in(own_key, 3), *heavy), -bound, bound).astype(kind)


def setup_inputs(seed: int = 0) -> dict:
    streams_of = jax.random.split(jax.random.key(seed), 7)
    tokens = centred(streams_of[0], (TOKENS, D), 1.0, 6.0, ((0, 8),))
    router_gates = jnp.clip(jnp.exp(math.log(1.0) - 2.3025851 * jax.random.uniform(streams_of[1], (TOKENS, TOP), jnp.float32) ** steps_of(streams_of[1], (TOKENS, TOP), ((0, 8),), -0.2, 0.2)), 0.1, 1.0)
    routes_keys = jax.random.split(jax.random.fold_in(streams_of[2], 1), TOKENS // TOK_DEV)
    routes_turns = jax.random.permutation(jax.random.fold_in(streams_of[2], 3), TOKENS // TOK_DEV)
    routes = jax.vmap(lambda own, number: shared_out(jax.random.fold_in(streams_of[2], 2), own, number, TOK_DEV, EXPERTS, TOP, CAP, 2))(routes_keys, routes_turns).reshape((TOKENS, TOP))
    gate_proj = centred(streams_of[3], (EXPERTS, D, FF), D ** -0.5, 0.09375, ((0, 8), (2, 16)))
    up_proj = centred(streams_of[4], (EXPERTS, D, FF), D ** -0.5, 0.09375, ((0, 8), (2, 16)))
    down_proj = gaussian_with(streams_of[5], (EXPERTS, FF, D), FF ** -0.5, 0.0625, ((0, 8), (1, 16)), (1, 2, 16, 2.0))
    return {"tokens": tokens, "router_gates": router_gates, "routes": routes, "gate_proj": gate_proj, "up_proj": up_proj, "down_proj": down_proj}


def slot_numbers(routes):
    grouped = routes.reshape(-1, TOK_DEV * TOP)
    chosen = (grouped[:, :, None] == jnp.arange(EXPERTS, dtype=jnp.int32)[None, None, :]).astype(jnp.int32)
    ranking = jnp.cumsum(chosen, axis=1) - chosen
    return jnp.sum(ranking * chosen, axis=2).reshape(-1, TOP).astype(jnp.int32)


def run_expert(operands):
    buffer_rows, gate_matrix, up_matrix, down_matrix = operands
    gate_act = jnp.dot(buffer_rows, gate_matrix, preferred_element_type=jnp.float32)
    up_act = jnp.dot(buffer_rows, up_matrix, preferred_element_type=jnp.float32)
    hidden = (jax.nn.silu(gate_act) * up_act).astype(jnp.bfloat16)
    shard_width = FF // N_FFN

    def add_shard(running, shard_index):
        hidden_part = lax.dynamic_slice_in_dim(hidden, shard_index * shard_width, shard_width, 1)
        down_part = lax.dynamic_slice_in_dim(down_matrix, shard_index * shard_width, shard_width, 0)
        rounded = jnp.dot(hidden_part, down_part, preferred_element_type=jnp.float32).astype(jnp.bfloat16)
        rounded = lax.optimization_barrier(rounded)
        return running + rounded.astype(jnp.float32), None

    start_sum = jnp.zeros((buffer_rows.shape[0], D), jnp.float32)
    result, unused = lax.scan(add_shard, start_sum, jnp.arange(N_FFN, dtype=jnp.int32))
    return result


def reference(tokens, router_gates, routes, gate_proj, up_proj, down_proj):
    sources = TOKENS // TOK_DEV
    slot = slot_numbers(routes)
    owner = (jnp.arange(TOKENS, dtype=jnp.int32) // TOK_DEV)[:, None]
    position = (owner * CAP + slot).astype(jnp.int32)
    buffers = jnp.zeros((EXPERTS, sources * CAP, D), jnp.bfloat16)
    buffers = buffers.at[routes, position].set(jnp.broadcast_to(tokens[:, None, :], (TOKENS, TOP, D)))
    outputs = lax.map(run_expert, (buffers, gate_proj, up_proj, down_proj))
    picked = outputs[routes, position]
    mixed = jnp.sum(router_gates[:, :, None] * picked, axis=1)
    return mixed.astype(jnp.bfloat16)
```

```python
import jax
import jax.numpy as jnp
from jax import lax
from jax.experimental import pallas as pl
from jax.experimental.pallas import tpu as pltpu
from jax.sharding import PartitionSpec as P

BLK = 256
HALF = 2 * BLK
CAP = 128
OWN_CHUNKS = ((0, 64), (64, 128))
PARTNER_CHUNKS = ((0, 64), (64, 128))
BF = jnp.bfloat16
F32 = jnp.float32


def LIMIT(mib):
    return pltpu.CompilerParams(vmem_limit_bytes=mib << 20)


VM = pl.BlockSpec(memory_space=pltpu.VMEM)
HB = pl.BlockSpec(memory_space=pltpu.HBM)


def y_shift(d):
    return [(y * 2 + x, ((y + d) % 4) * 2 + x) for y in range(4) for x in range(2)]


X_LO = [(i, i ^ 1) for i in range(8)]
SWAP = [(i, i ^ 1) for i in range(16)]
Z_PAIR_A = [(z * 4 + r, (z ^ 1) * 4 + r) for z in range(4) for r in range(4)]
Z_PAIR_B = [(z * 4 + r, (3 - z) * 4 + r) for z in range(4) for r in range(4)]


def final_perm(dx, dz):
    return [
        (z * 4 + x * 2 + c, (z ^ (2 * dz)) * 4 + (x ^ dx) * 2 + c)
        for z in range(4)
        for x in range(2)
        for c in range(2)
    ]


def places():
    e = lax.axis_index("expert")
    f = lax.axis_index("ffn")
    return e // 2, e % 2, f // 4, (f // 2) % 2, f % 2


def block_id(j, z, core):
    parity = (z % 2 + j // 4 % 2) % 2
    return (parity + 2 * (j % 2)) * 4 + (j // 2 % 2) * 2 + (core + j // 8) % 2


def slot_rows(rg, y, x):
    expert = ((y + lax.broadcasted_iota(jnp.int32, (8, 256), 0)) % 4 * 2 + x).astype(F32)
    first = rg[0:1, :] == expert
    second = rg[1:2, :] == expert
    named = jnp.where(first | second, 1.0, 0.0)
    earlier = jnp.where(
        lax.broadcasted_iota(jnp.int32, (256, 256), 0) < lax.broadcasted_iota(jnp.int32, (256, 256), 1), 1.0, 0.0
    ).astype(BF)
    count = jnp.dot(named.astype(BF), earlier, preferred_element_type=F32)
    slots = jnp.where(named > 0.5, count, -1.0)
    gates = jnp.where(first, rg[2:3, :], 0.0) + jnp.where(second, rg[3:4, :], 0.0)
    return slots, gates


def is_slot(slots, r, lo, hi):
    ids = (lax.broadcasted_iota(jnp.int32, (hi - lo, 256), 0) + lo).astype(F32)
    return ids == slots[r : r + 1, :]


def place_blocks(rg, tok, y, x, chunks, outs):
    slots, _ = slot_rows(rg, y, x)
    i = 0
    for lo, hi in chunks:
        for r in range(4):
            one_hot = jnp.where(is_slot(slots, r, lo, hi), 1.0, 0.0).astype(BF)
            outs[i][...] = jnp.dot(one_hot, tok, preferred_element_type=F32).astype(BF)
            i += 1


def block_shapes(chunks):
    return [jax.ShapeDtypeStruct((hi - lo, 4 * BLK), BF) for lo, hi in chunks for _ in range(4)]


def split4(outs, chunks):
    return [list(outs[4 * i : 4 * i + 4]) for i in range(len(chunks))]


def cost(flops, nbytes):
    return pl.CostEstimate(flops=int(flops), bytes_accessed=int(nbytes), transcendentals=0)


def place_own(rg, tokens):
    def kernel(rg_ref, tok_hbm, col_ref, *rest):
        outs, sem = rest[:-1], rest[-1]
        y, x, z, _, core = places()
        copies = []
        for j in range(4):
            at = pl.multiple_of(block_id(j, z, core) * BLK, BLK)
            cp = pltpu.make_async_copy(
                tok_hbm.at[:, pl.ds(at, BLK)], col_ref.at[:, pl.ds(j * BLK, BLK)], sem.at[j]
            )
            cp.start()
            copies.append(cp)
        for cp in copies:
            cp.wait()
        place_blocks(rg_ref[...], col_ref[...], y, x, OWN_CHUNKS, outs)

    shapes = [jax.ShapeDtypeStruct((256, 4 * BLK), BF)] + block_shapes(OWN_CHUNKS)
    outs = pl.pallas_call(
        kernel,
        name="place_own",
        out_shape=shapes,
        in_specs=[VM, HB],
        out_specs=[VM] * len(shapes),
        scratch_shapes=[pltpu.SemaphoreType.DMA((4,))],
        cost_estimate=cost(2 * 512 * 256 * 1024, 2 << 20),
        compiler_params=LIMIT(4),
    )(rg, tokens)
    return outs[0], split4(outs[1:], OWN_CHUNKS)


def place_partner(rg, tok):
    def kernel(rg_ref, tok_ref, *outs):
        y, x, _, _, _ = places()
        place_blocks(rg_ref[...], tok_ref[...], y, x, PARTNER_CHUNKS, outs)

    shapes = block_shapes(PARTNER_CHUNKS)
    outs = pl.pallas_call(
        kernel,
        name="place_partner",
        out_shape=shapes,
        in_specs=[VM, VM],
        out_specs=[VM] * len(shapes),
        cost_estimate=cost(2 * 512 * 256 * 1024, 2 << 20),
        compiler_params=LIMIT(4),
    )(rg, tok)
    return split4(outs, PARTNER_CHUNKS)


def load_weights(gate, up, down):
    width, hidden = gate.shape

    def kernel(g_hbm, u_hbm, d_hbm, g_ref, u_ref, d_ref, sem):
        _, _, z, _, core = places()
        copies = []
        for j in range(16):
            at = pl.multiple_of(block_id(j, z, core) * BLK, BLK)
            to = pl.ds(j * BLK, BLK)
            copies.append(pltpu.make_async_copy(g_hbm.at[pl.ds(at, BLK), :], g_ref.at[to, :], sem.at[3 * j]))
            copies.append(pltpu.make_async_copy(u_hbm.at[pl.ds(at, BLK), :], u_ref.at[to, :], sem.at[3 * j + 1]))
            copies.append(pltpu.make_async_copy(d_hbm.at[:, pl.ds(at, BLK)], d_ref.at[:, to], sem.at[3 * j + 2]))
        for cp in copies:
            cp.start()
        for cp in copies:
            cp.wait()

    return pl.pallas_call(
        kernel,
        name="load_weights",
        out_shape=[
            pltpu.VMEM((width, hidden), BF),
            pltpu.VMEM((width, hidden), BF),
            pltpu.VMEM((hidden, width), BF),
        ],
        in_specs=[HB] * 3,
        out_specs=[VM] * 3,
        scratch_shapes=[pltpu.SemaphoreType.DMA((48,))],
        cost_estimate=cost(5e9, 44 << 20),
        compiler_params=LIMIT(4),
    )(gate, up, down)


def join(parts):
    rows = parts[0].shape[0]

    def kernel(a, b, c, d, all_ref, a_ref, b_ref):
        for i, part in enumerate((a, b, c, d)):
            at = pl.ds(i * rows, rows)
            all_ref[at, :] = part[...]
            a_ref[at, :] = part[:, :HALF]
            b_ref[at, :] = part[:, HALF:]

    return pl.pallas_call(
        kernel,
        name="join",
        out_shape=[
            jax.ShapeDtypeStruct((4 * rows, 4 * BLK), BF),
            jax.ShapeDtypeStruct((4 * rows, HALF), BF),
            jax.ShapeDtypeStruct((4 * rows, HALF), BF),
        ],
        in_specs=[VM] * 4,
        out_specs=[VM] * 3,
        cost_estimate=cost(3e8, 1 << 20),
        compiler_params=LIMIT(4),
    )(*parts)


def expert(xs, weights):
    rows = xs[0].shape[0]
    width, hidden = weights[0].shape
    full = hidden // BLK * BLK

    def kernel(*refs):
        x, (wg, wu, wd, send, keep, hid) = refs[:6], refs[6:]

        def gate_like(pick):
            acc, at = None, 0
            for ref in x:
                k = ref.shape[1]
                part = jnp.dot(ref[...], pick(pl.ds(at, k)), preferred_element_type=F32)
                acc = part if acc is None else acc + part
                at += k
            return acc

        def put(n, size, g, u):
            hid[:, n : n + size] = (g / (1.0 + jnp.exp(-g)) * u).astype(BF)

        for n in range(0, full, BLK):
            g = gate_like(lambda k: wg[k, n : n + BLK])
            u = gate_like(lambda k: wu[k, n : n + BLK])
            put(n, BLK, g, u)
        if full < hidden:
            left = hidden - full
            both = gate_like(lambda k: jnp.concatenate([wg[k, full:], wu[k, full:]], axis=1))
            put(full, left, both[:, :left], both[:, left:])
        h = hid[...]
        for j in range(width // HALF):
            to, at = (send, j) if j < width // HALF // 2 else (keep, j - width // HALF // 2)
            col = (j + width // HALF // 2) % (width // HALF) * HALF
            out = jnp.dot(h, wd[:, col : col + HALF], preferred_element_type=F32)
            to[:, at * HALF : (at + 1) * HALF] = out.astype(BF)

    return pl.pallas_call(
        kernel,
        name="expert",
        out_shape=[jax.ShapeDtypeStruct((rows, width // 2), BF)] * 2,
        in_specs=[VM] * 9,
        out_specs=[VM] * 2,
        scratch_shapes=[pltpu.VMEM((rows, hidden), BF)],
        cost_estimate=cost(6 * rows * width * hidden, 4 << 20),
        compiler_params=LIMIT(16),
    )(*xs, *weights)


def add_pair(keep, got):
    rows = keep.shape[0]

    def kernel(keep_ref, got_ref, own, a, b):
        def total(lo, hi):
            return (keep_ref[:, lo:hi].astype(F32) + got_ref[:, lo:hi].astype(F32)).astype(BF)

        a[...] = total(2 * HALF, 3 * HALF)
        b[...] = total(3 * HALF, 4 * HALF)
        own[...] = total(0, 2 * HALF)

    return pl.pallas_call(
        kernel,
        name="add_pair",
        out_shape=[
            jax.ShapeDtypeStruct((rows, 2 * HALF), BF),
            jax.ShapeDtypeStruct((rows, HALF), BF),
            jax.ShapeDtypeStruct((rows, HALF), BF),
        ],
        in_specs=[VM] * 2,
        out_specs=[VM] * 3,
        cost_estimate=cost(5e8, 2 << 20),
        compiler_params=LIMIT(4),
    )(keep, got)


def add_z(own, a, b):
    rows = own.shape[0] // 4

    def kernel(own_ref, a_ref, b_ref, *outs):
        for i, out in enumerate(outs):
            at = pl.ds(i * rows, rows)
            out[:, :HALF] = (own_ref[at, :HALF].astype(F32) + a_ref[at, :].astype(F32)).astype(BF)
            out[:, HALF:] = (own_ref[at, HALF:].astype(F32) + b_ref[at, :].astype(F32)).astype(BF)

    return pl.pallas_call(
        kernel,
        name="add_z",
        out_shape=[jax.ShapeDtypeStruct((rows, 2 * HALF), BF)] * 4,
        in_specs=[VM] * 3,
        out_specs=[VM] * 4,
        cost_estimate=cost(3e8, 1 << 20),
        compiler_params=LIMIT(4),
    )(own, a, b)


def mix_rows(rg, y, x, chunks, refs):
    slots, gates = slot_rows(rg, y, x)
    weights, rows = [], []
    for i, (lo, hi) in enumerate(chunks):
        for r in range(4):
            weights.append(jnp.where(is_slot(slots, r, lo, hi), gates[r : r + 1, :], 0.0).astype(BF))
            rows.append(refs[4 * i + r][...])
    return lax.dot_general(
        jnp.concatenate(weights, axis=0),
        jnp.concatenate(rows, axis=0),
        (((0,), (0,)), ((), ())),
        preferred_element_type=F32,
    )


def mix_partner(rg, rows):
    def kernel(rg_ref, *refs):
        y, x, _, _, _ = places()
        refs[-1][...] = mix_rows(rg_ref[...], y, x, PARTNER_CHUNKS, refs[:-1]).astype(BF)

    return pl.pallas_call(
        kernel,
        name="mix_partner",
        out_shape=jax.ShapeDtypeStruct((256, 4 * BLK), BF),
        in_specs=[VM] * (1 + len(rows)),
        out_specs=VM,
        cost_estimate=cost(1e9, 1 << 20),
        compiler_params=LIMIT(4),
    )(rg, *rows)


def mix_own(rg, rows, other):
    def kernel(rg_ref, other_ref, *rest):
        refs, outs, tmp = rest[: len(rows)], rest[len(rows) : -1], rest[-1]
        y, x, z, x_hi, _ = places()
        tmp[...] = mix_rows(rg_ref[...], y, x, OWN_CHUNKS, refs) + other_ref[...].astype(F32)
        for dx in range(2):
            for dz in range(2):
                at = pl.multiple_of(((x_hi + dx) % 2 * 2 + (z // 2 + dz) % 2) * BLK, BLK)
                outs[2 * dx + dz][...] = tmp[:, pl.ds(at, BLK)].astype(BF)

    return pl.pallas_call(
        kernel,
        name="mix_own",
        out_shape=[jax.ShapeDtypeStruct((256, BLK), BF)] * 4,
        in_specs=[VM] * (2 + len(rows)),
        out_specs=[VM] * 4,
        scratch_shapes=[pltpu.VMEM((256, 4 * BLK), F32)],
        cost_estimate=cost(1e9, 1 << 20),
        compiler_params=LIMIT(4),
    )(rg, other, *rows)


def per_device(tokens, router_gates, routes, gate_proj, up_proj, down_proj):
    rg = jnp.concatenate([routes.T.astype(F32), router_gates.T], axis=0)
    rg_partner = lax.ppermute(rg, "expert", X_LO)
    cols, own = place_own(rg, tokens)
    cols_partner = lax.ppermute(cols, "expert", X_LO)
    weights = load_weights(gate_proj[0], up_proj[0], down_proj[0])
    partner = place_partner(rg_partner, cols_partner)

    def dispatch(blocks):
        parts = [blocks[0]] + [lax.ppermute(blocks[d], "expert", y_shift(d)) for d in (1, 2, 3)]
        joined, a, b = join(parts)
        za = lax.ppermute(a, "ffn", Z_PAIR_A)
        zb = lax.ppermute(b, "ffn", Z_PAIR_B)
        mine = [joined, za, zb]
        return mine + [lax.ppermute(v, "ffn", SWAP) for v in mine]

    def combine(send, keep):
        own_sum, a, b = add_pair(keep, lax.ppermute(send, "ffn", SWAP))
        a = lax.ppermute(a, "ffn", Z_PAIR_A)
        b = lax.ppermute(b, "ffn", Z_PAIR_B)
        rows = add_z(own_sum, a, b)
        return [rows[0]] + [lax.ppermute(rows[d], "expert", y_shift(-d)) for d in (1, 2, 3)]

    back_own, back_partner = [], []
    order = [(own[0], back_own)] + [(b, back_partner) for b in partner] + [(b, back_own) for b in own[1:]]
    ready = [dispatch(blocks) for blocks, _ in order]
    for xs, (_, back) in zip(ready, order):
        back += combine(*expert(xs, weights))
    other = lax.ppermute(mix_partner(rg_partner, back_partner), "expert", X_LO)
    outs = mix_own(rg, back_own, other)
    total = outs[0].astype(F32)
    for dx, dz in ((0, 1), (1, 0), (1, 1)):
        total = total + lax.ppermute(outs[2 * dx + dz], "ffn", final_perm(dx, dz)).astype(F32)
    return total.astype(BF)


def solution(mesh):
    in_specs = (
        P("expert", None),
        P("expert", None),
        P("expert", None),
        P("expert", None, "ffn"),
        P("expert", None, "ffn"),
        P("expert", "ffn", None),
    )
    return jax.shard_map(
        per_device, mesh=mesh, in_specs=in_specs, out_specs=P("expert", "ffn"), check_vma=False
    )
```

```python
import jax
import jax.numpy as jnp
from jax import lax
from jax.experimental import pallas as pl
from jax.experimental.pallas import tpu as pltpu
from jax.sharding import PartitionSpec as P

BLK = 256
HALF = 2 * BLK
QUARTER = 4 * BLK
CAP = 128
SENT = ((0, 2, 4, 6), (1, 3, 5, 7))
DONE = ((0, 0, 128), (1, 0, 64), (1, 64, 128))
BACK = ((0,), (1,), (2,))
X_LO = [(i, i ^ 1) for i in range(8)]
BF = jnp.bfloat16
F32 = jnp.float32
VM = pl.BlockSpec(memory_space=pltpu.VMEM)
HB = pl.BlockSpec(memory_space=pltpu.HBM)
SWAP = [(i, i ^ 1) for i in range(16)]
Z_PAIR_A = [(z * 4 + r, (z ^ 1) * 4 + r) for z in range(4) for r in range(4)]
Z_PAIR_B = [(z * 4 + r, (3 - z) * 4 + r) for z in range(4) for r in range(4)]


def final_perm(dx, dz):
    return [
        (z * 4 + x * 2 + c, (z ^ (2 * dz)) * 4 + (x ^ dx) * 2 + c)
        for z in range(4)
        for x in range(2)
        for c in range(2)
    ]


def permute(value, perm):
    return lax.ppermute(value, "ffn", perm)


def shift(r, sign):
    return [(y * 2 + x, (y + sign * (r // 2)) % 4 * 2 + (x ^ r % 2)) for y in range(4) for x in range(2)]


def exchange(distances, blocks, sign):
    moved = []
    for r, block in zip(distances, blocks):
        if r:
            block = lax.ppermute(block, "expert", shift(r, sign))
        moved.append(block)
    return moved


def kernel_call(kernel, outs, in_specs, flops, mib, *args, scratch=()):
    several = isinstance(outs, list)
    return pl.pallas_call(
        kernel,
        out_shape=outs,
        in_specs=in_specs,
        out_specs=[VM] * len(outs) if several else VM,
        scratch_shapes=list(scratch),
        cost_estimate=pl.CostEstimate(flops=int(flops), bytes_accessed=1 << 20, transcendentals=0),
        compiler_params=pltpu.CompilerParams(vmem_limit_bytes=mib << 20),
    )(*args)


def shape(*dims, dtype=BF):
    return jax.ShapeDtypeStruct(dims, dtype)


def places():
    f = lax.axis_index("ffn")
    return f // 4, (f // 2) % 2, f % 2


def home():
    e = lax.axis_index("expert")
    return e // 2, e % 2


def quarter_start(i, z, core):
    return pl.multiple_of(((z + i % 2) % 2 * 2 + (core + i // 2) % 2) * QUARTER, QUARTER)


def out_start(j, z, core):
    parity = (z % 2 + j // 4 % 2) % 2
    block = (parity + 2 * (j % 2)) * 4 + (j // 2 % 2) * 2 + (core + j // 8) % 2
    return pl.multiple_of(block * BLK, BLK)


def slot_rows(routes, gates, neighbour=0):
    y, x = home()
    r = lax.broadcasted_iota(jnp.int32, (8, 256), 0)
    expert = ((y + r // 2) % 4 * 2 + (x + neighbour + r) % 2).astype(F32)
    first = routes[0:1, :] == expert
    second = routes[1:2, :] == expert
    named = jnp.where(first | second, 1.0, 0.0)
    earlier = jnp.where(
        lax.broadcasted_iota(jnp.int32, (256, 256), 0) < lax.broadcasted_iota(jnp.int32, (256, 256), 1), 1.0, 0.0
    ).astype(BF)
    count = jnp.dot(named.astype(BF), earlier, preferred_element_type=F32)
    slots = jnp.where(named > 0.5, count, -1.0)
    if gates is None:
        return slots, None
    return slots, jnp.where(first, gates[0:1, :], 0.0) + jnp.where(second, gates[1:2, :], 0.0)


def is_slot(slots, e, lo, hi):
    ids = (lax.broadcasted_iota(jnp.int32, (hi - lo, 256), 0) + lo).astype(F32)
    return ids == slots[e : e + 1, :]


def put_blocks(slots, distances, cols, outs):
    picks = [jnp.where(is_slot(slots, r, 0, CAP), 1.0, 0.0).astype(BF) for r in distances]
    rows = jnp.dot(jnp.concatenate(picks, axis=0), cols, preferred_element_type=F32).astype(BF)
    for i, out in enumerate(outs):
        out[...] = rows[i * CAP : (i + 1) * CAP, :]


def place(routes, tokens):
    def kernel(routes_ref, tok_hbm, cols, *rest):
        outs, sem = rest[:-1], rest[-1]
        z, _, core = places()
        cp = pltpu.make_async_copy(
            tok_hbm.at[:, pl.ds(quarter_start(0, z, core), QUARTER)], cols.at[pl.ds(0, 256), :], sem
        )
        cp.start()
        given = routes_ref[...].astype(F32)
        spread = jnp.concatenate([given[0:1, :], given[1:2, :], jnp.zeros((1, QUARTER - 512), F32)], axis=1)
        cols[256:272, :] = jnp.broadcast_to(spread, (16, QUARTER)).astype(BF)
        slots, _ = slot_rows(given, None)
        cp.wait()
        put_blocks(slots, SENT[0], cols[0:256, :], outs)

    return kernel_call(
        kernel, [shape(272, QUARTER)] + [shape(CAP, QUARTER)] * 4, [VM, HB], 3e8, 4, routes, tokens,
        scratch=[pltpu.SemaphoreType.DMA],
    )


def place_neighbour(cols):
    def kernel(cols_ref, *outs):
        given = cols_ref[256:272, :].astype(F32)
        routes = jnp.concatenate([given[0:1, 0:256], given[0:1, 256:512]], axis=0)
        slots, _ = slot_rows(routes, None, 1)
        put_blocks(slots, SENT[1], cols_ref[0:256, :], outs)

    return kernel_call(kernel, [shape(CAP, QUARTER)] * 4, [VM], 3e8, 4, cols)


def join(blocks):
    n, count = blocks[0].shape[0], len(blocks)

    def kernel(*refs):
        srcs, (rows, a, b) = refs[:count], refs[count:]
        for i, src in enumerate(srcs):
            at = pl.ds(i * n, n)
            rows[at, :] = src[...]
            a[at, :] = src[:, :HALF]
            b[at, :] = src[:, HALF:]

    outs = [shape(count * n, QUARTER), shape(count * n, HALF), shape(count * n, HALF)]
    return kernel_call(kernel, outs, [VM] * count, 3e8, 2, *blocks)


def column_tile(wg, wu, k, c):
    hidden = wg.shape[1]
    full = hidden // BLK * BLK
    if c < full:
        return wg[k, c : c + BLK]
    if c < 2 * full:
        return wu[k, c - full : c - full + BLK]
    return jnp.concatenate([wg[k, full:], wu[k, full:]], axis=1)


def start_expert(mine, other, weights, loads):
    rows, (width, hidden) = mine.shape[0], weights[0].shape

    def multiply(mine_ref, other_ref, wg, wu, acc, ready):
        for i, ref in ((0, mine_ref), (2, other_ref)):
            ready(i)

            @pl.loop(0, rows // 256)
            def _(half):
                at = pl.ds(pl.multiple_of(half * 256, 256), 256)
                for c in range(0, 2 * hidden, BLK):
                    tile = column_tile(wg, wu, pl.ds(i * QUARTER, QUARTER), c)
                    part = jnp.dot(ref[at, :], tile, preferred_element_type=F32)
                    acc[at, c : c + BLK] = part if i == 0 else acc[at, c : c + BLK] + part


    if not loads:

        def plain(mine_ref, other_ref, wg, wu, acc):
            multiply(mine_ref, other_ref, wg, wu, acc, lambda i: None)

        acc = shape(rows, 2 * hidden, dtype=F32)
        return kernel_call(plain, acc, [VM] * 4, 3 * rows * width * hidden, 4, mine, other, *weights[:2]), weights

    def kernel(mine_ref, other_ref, g_hbm, u_hbm, d_hbm, acc, wg, wu, wd, sem):
        z, _, core = places()
        copies = []
        for i in (0, 2, 1, 3):
            at, to = pl.ds(quarter_start(i, z, core), QUARTER), pl.ds(i * QUARTER, QUARTER)
            copies.append(pltpu.make_async_copy(g_hbm.at[at, :], wg.at[to, :], sem.at[2 * i]))
            copies.append(pltpu.make_async_copy(u_hbm.at[at, :], wu.at[to, :], sem.at[2 * i + 1]))
        for j in range(16):
            at, to = pl.ds(out_start(j, z, core), BLK), pl.ds(j * BLK, BLK)
            copies.append(pltpu.make_async_copy(d_hbm.at[:, at], wd.at[:, to], sem.at[8 + j]))
        for cp in copies:
            cp.start()

        def ready(i):
            copies[i].wait()
            copies[i + 1].wait()

        multiply(mine_ref, other_ref, wg, wu, acc, ready)
        for cp in copies[4:]:
            cp.wait()

    outs = [shape(rows, 2 * hidden, dtype=F32)] + [pltpu.VMEM(w.shape, BF) for w in weights]
    got = kernel_call(
        kernel, outs, [VM, VM, HB, HB, HB], 3 * rows * width * hidden, 4, mine, other, *weights,
        scratch=[pltpu.SemaphoreType.DMA((24,))],
    )
    return got[0], got[1:]


def expert(xs, lo, hi, weights, acc):
    width, hidden = weights[0].shape
    full = hidden // BLK * BLK
    left = hidden - full
    count = xs[0].shape[0] // CAP
    rows = count * (hi - lo)

    def kernel(*refs):
        x, (wg, wu, wd, acc_ref, send, keep, hid) = refs[:4], refs[4:]

        def gate_up(rows_of, c):
            total = rows_of(acc_ref, slice(c, c + BLK))
            for i, ref in enumerate(x):
                at = pl.ds((i // 2 * 2 + 1) * QUARTER + i % 2 * HALF, HALF)
                tile = column_tile(wg, wu, at, c)
                total = total + jnp.dot(rows_of(ref, slice(None)), tile, preferred_element_type=F32)
            return total

        def run(rows_of, to):
            def put(c, size, g, u):
                hid[:, c : c + size] = (g / (1.0 + jnp.exp(-g)) * u).astype(BF)

            for c in range(0, full, BLK):
                put(c, BLK, gate_up(rows_of, c), gate_up(rows_of, full + c))
            both = gate_up(rows_of, 2 * full)
            put(full, left, both[:, :left], both[:, left:])
            h = hid[...]
            for c in range(0, width, HALF):
                at = (c + width // 2) % width
                out = jnp.dot(h, wd[:, at : at + HALF], preferred_element_type=F32).astype(BF)
                if at < width // 2:
                    keep[to, at : at + HALF] = out
                else:
                    send[to, at - width // 2 : at - width // 2 + HALF] = out

        def some(ref, cols):
            return jnp.concatenate([ref[s * CAP + lo : s * CAP + hi, cols] for s in range(count)], axis=0)

        if hi - lo < CAP:
            run(some, slice(None))
        else:

            @pl.loop(0, rows // 256)
            def _(i):
                at = pl.ds(pl.multiple_of(i * 256, 256), 256)
                run(lambda ref, cols: ref[at, cols], at)

    args = [xs[1], xs[2], xs[4], xs[5], *weights, acc]
    return kernel_call(
        kernel, [shape(rows, width // 2)] * 2, [VM] * len(args), 6 * rows * width * hidden, 8, *args,
        scratch=[pltpu.VMEM((256, hidden), BF)],
    )


def add_pair(keep, got):
    rows = keep.shape[0]

    def kernel(keep_ref, got_ref, own, a, b):
        def total(lo, hi):
            return (keep_ref[:, lo:hi].astype(F32) + got_ref[:, lo:hi].astype(F32)).astype(BF)

        a[...] = total(2 * HALF, 3 * HALF)
        b[...] = total(3 * HALF, 4 * HALF)
        own[...] = total(0, 2 * HALF)

    outs = [shape(rows, QUARTER), shape(rows, HALF), shape(rows, HALF)]
    return kernel_call(kernel, outs, [VM] * 2, 5e8, 4, keep, got)


def add_z(parts):
    count = len(SENT[0])
    sizes = [own.shape[0] // count for own, _, _ in parts]

    def kernel(*refs):
        outs = refs[3 * len(parts) :]
        for r, out in enumerate(outs):
            done = 0
            for i, n in enumerate(sizes):
                own, a, b = refs[3 * i : 3 * i + 3]
                at, to = pl.ds(r * n, n), pl.ds(done, n)
                out[to, :HALF] = (own[at, :HALF].astype(F32) + a[at, :].astype(F32)).astype(BF)
                out[to, HALF:] = (own[at, HALF:].astype(F32) + b[at, :].astype(F32)).astype(BF)
                done += n

    flat = [v for part in parts for v in part]
    return kernel_call(kernel, [shape(sum(sizes), QUARTER)] * count, [VM] * len(flat), 3e8, 4, *flat)


def mix(routes, gates, rows):
    def kernel(routes_ref, gates_ref, *rest):
        refs, outs, tmp = rest[: len(rows)], rest[len(rows) : -1], rest[-1]
        z, x_hi, _ = places()
        slots, weight = slot_rows(routes_ref[...].astype(F32), gates_ref[...])
        total, done = None, 0
        for calls in BACK:
            parity, lo, hi = DONE[calls[0]][0], DONE[calls[0]][1], DONE[calls[-1]][2]
            mine = jnp.concatenate([ref[...] for ref in refs[done : done + len(SENT[parity])]], axis=0)
            done += len(SENT[parity])
            w = jnp.concatenate(
                [jnp.where(is_slot(slots, r, lo, hi), weight[r : r + 1, :], 0.0).astype(BF) for r in SENT[parity]],
                axis=0,
            )
            part = lax.dot_general(w, mine, (((0,), (0,)), ((), ())), preferred_element_type=F32)
            total = part if total is None else total + part
        tmp[...] = total
        for dx in range(2):
            for dz in range(2):
                at = pl.multiple_of(((x_hi + dx) % 2 * 2 + (z // 2 + dz) % 2) * BLK, BLK)
                outs[2 * dx + dz][...] = tmp[:, pl.ds(at, BLK)].astype(BF)

    return kernel_call(
        kernel, [shape(256, BLK)] * 4, [VM] * (2 + len(rows)), 1e9, 6, routes, gates, *rows,
        scratch=[pltpu.VMEM((256, QUARTER), F32)],
    )


def last_sum(parts):
    def kernel(a, b, c, d, out):
        out[...] = (a[...].astype(F32) + b[...].astype(F32) + c[...].astype(F32) + d[...].astype(F32)).astype(BF)

    return kernel_call(kernel, shape(*parts[0].shape), [VM] * 4, 1e8, 2, *parts)


def per_device(tokens, router_gates, routes, gate_proj, up_proj, down_proj):
    routes, gates = routes.T, router_gates.T
    weights = [pltpu.with_memory_space_constraint(w[0], pltpu.HBM) for w in (gate_proj, up_proj, down_proj)]
    tokens = pltpu.with_memory_space_constraint(tokens, pltpu.HBM)
    placed = place(routes, tokens)

    def dispatch(blocks):
        rows, a, b = join(exchange(SENT[0], blocks, 1))
        mine = [rows, permute(a, Z_PAIR_A), permute(b, Z_PAIR_B)]
        return mine + [permute(v, SWAP) for v in mine]

    cols = lax.ppermute(placed[0], "expert", X_LO)
    ready = [dispatch(placed[1:]), dispatch(place_neighbour(cols))]
    accs = []
    for k, xs in enumerate(ready):
        acc, weights = start_expert(xs[0], xs[3], weights, k == 0)
        accs.append(acc)
    parts = []
    for k, lo, hi in DONE:
        send, keep = expert(ready[k], lo, hi, weights, accs[k])
        own, a, b = add_pair(keep, permute(send, SWAP))
        parts.append((own, permute(a, Z_PAIR_A), permute(b, Z_PAIR_B)))
    back = []
    for calls in BACK:
        rows = add_z([parts[i] for i in calls])
        back += exchange(SENT[DONE[calls[0]][0]], rows, -1)
    outs = mix(routes, gates, back)
    moved = [outs[0]]
    for dx, dz in ((0, 1), (1, 0), (1, 1)):
        moved.append(permute(outs[2 * dx + dz], final_perm(dx, dz)))
    return last_sum(moved)


def solution(mesh):
    in_specs = (
        P("expert", None),
        P("expert", None),
        P("expert", None),
        P("expert", None, "ffn"),
        P("expert", None, "ffn"),
        P("expert", "ffn", None),
    )
    return jax.shard_map(per_device, mesh=mesh, in_specs=in_specs, out_specs=P("expert", "ffn"), check_vma=False)
```
